32 devices in a mesh: blk: 16 (over z, y, core), head: 2 (over x).
Axes of the slice: x: 2, y: 2, z: 4, core: 2. Of those that a mesh axis runs over, the one named last changes fastest.
Arguments:
- queries: bfloat16 [8192, 16, 128], P('blk', 'head'), may hold values from -6 to 6
- out_grad: bfloat16 [8192, 16, 128], P('blk', 'head'), may hold values from -6 to 6
- outputs: bfloat16 [8192, 16, 128], P('blk', 'head'), may hold values from -6 to 6
- key_vectors: bfloat16 [8192, 128], P('blk'), may hold values from -6 to 6
- value_vectors: bfloat16 [8192, 128], P('blk'), may hold values from -6 to 6
- logsumexp: float32 [8192, 16], P('blk', 'head'), may hold values from 4 to 7
- positions: int32 [8192], P('blk'), may hold values from 0 to 8191, as said below
- doc_start: int32 [8192], P('blk'), may hold values from 0 to 8191, as said below
Outputs:
- query_grad: bfloat16 [8192, 16, 128], P('blk', 'head')
- key_grad: bfloat16 [8192, 128], P('blk')
- value_grad: bfloat16 [8192, 128], P('blk')
The draws below stay inside these ranges and needn't reach their ends.
Inputs may be any that keep to these rules, and one draw needn't show every extreme that they name: positions is a permutation of 0 to 8191; row r holds position (r mod 512) * 16 + sigma(r div 512), sigma a permutation of the blocks of 512 rows. doc_start of a row is the first position of the document that holds the row's position; documents are runs of consecutive positions, the first starting at 0, and the last position starts a document of its own.
All inputs are finite; a program needn't handle non-finite values.
Results may differ from the reference program's by a relative error of at most 0.0063.
Values may be sent and summed in bfloat16 or wider, within the bound.
A program may use at most 64 MiB of HBM per device.

```python
import jax
import jax.numpy as jnp
from jax import lax

HQ = 16
HD = 128
TOK_DEV = 512
STEPS = 4
SEQ = 8192
N_BLK = 16


def shared_positions(key):
    sub_key = jax.random.fold_in(key, 11)
    block_order = jax.random.permutation(sub_key, N_BLK).astype(jnp.int32)
    row_ids = jnp.arange(SEQ, dtype=jnp.int32)
    return (row_ids % TOK_DEV * N_BLK + block_order[row_ids // TOK_DEV]).astype(jnp.int32)


def draw_positions(key, part):
    return shared_positions(key)


def draw_doc_start(key, part):
    places = shared_positions(key)
    doc_flags = jax.random.randint(jax.random.fold_in(key, 12), (SEQ,), 0, max(SEQ // 8, 2)) == 0
    cell_ids = jnp.arange(SEQ, dtype=jnp.int32)
    start_marks = jnp.where(doc_flags | (cell_ids == 0) | (cell_ids == SEQ - 1), cell_ids, 0).astype(jnp.int32)
    doc_starts = lax.cummax(start_marks, axis=0)
    return doc_starts[places].astype(jnp.int32)


def levels(key, shape, pieces, least, high):
    level, own = 1.0, jax.random.fold_in(key, 6)
    for axis_at, shards_of in pieces:
        steps = jnp.exp(jax.random.uniform(jax.random.fold_in(own, axis_at), (shards_of,), jnp.float32, least / len(pieces), high / len(pieces)))
        level = level * jnp.repeat(steps, shape[axis_at] // shards_of).reshape([-1 if axis == axis_at else 1 for axis in range(len(shape))])
    return level


def normal_values(rng, extent, width, reach, cuts=(), kind=jnp.bfloat16):
    result = width * jax.random.normal(rng, extent, jnp.float32)
    if cuts:
        result = result * levels(rng, extent, cuts, -0.22, 0.18)
    return jnp.clip(result, -reach, reach).astype(kind)


def setup_inputs(seed: int = 0) -> dict:
    key_of = jax.random.split(jax.random.key(seed), 9)
    return {
        "queries": normal_values(key_of[0], (SEQ, HQ, HD), 1.0, 6.0, ((0, 16), (1, 2))),
        "out_grad": normal_values(key_of[1], (SEQ, HQ, HD), 1.0, 6.0, ((0, 16), (1, 2))),
        "outputs": normal_values(key_of[2], (SEQ, HQ, HD), 1.0, 6.0, ((0, 16), (1, 2))),
        "key_vectors": normal_values(key_of[3], (SEQ, HD), 1.0, 6.0, ((0, 16),)),
        "value_vectors": normal_values(key_of[4], (SEQ, HD), 1.0, 6.0, ((0, 16),)),
        "logsumexp": jnp.clip(4.0 + 3.0 * jax.random.uniform(key_of[5], (SEQ, HQ), jnp.float32) ** levels(key_of[5], (SEQ, HQ), ((0, 16), (1, 2)), -0.2, 0.2), 4.0, 7.0),
        "positions": draw_positions(jax.random.fold_in(key_of[8], 71), 0),
        "doc_start": draw_doc_start(jax.random.fold_in(key_of[8], 71), 0),
    }


def block_grads(queries, out_grad, logsumexp, row_delta, query_places, query_starts, key_vectors, value_vectors, key_places):
    scaling = HD ** -0.5
    query_wide = queries.astype(jnp.float32)
    grad_wide = out_grad.astype(jnp.float32)
    key_wide = key_vectors.astype(jnp.float32)
    value_wide = value_vectors.astype(jnp.float32)
    scores = jnp.einsum("thd,kd->htk", query_wide, key_wide) * scaling
    allowed = (key_places[None, :] <= query_places[:, None]) & (key_places[None, :] >= query_starts[:, None])
    attend = jnp.where(allowed[None], jnp.exp(scores - logsumexp.T[:, :, None]), jnp.float32(0.0))
    attend_low = lax.optimization_barrier(attend.astype(jnp.bfloat16)).astype(jnp.float32)
    attend_grad = jnp.einsum("thd,kd->htk", grad_wide, value_wide)
    score_grad = attend * (attend_grad - row_delta.T[:, :, None])
    score_low = lax.optimization_barrier(score_grad.astype(jnp.bfloat16)).astype(jnp.float32)
    value_part = jnp.einsum("htk,thd->kd", attend_low, grad_wide)
    key_part = scaling * jnp.einsum("htk,thd->kd", score_low, query_wide)
    query_part = scaling * jnp.einsum("htk,kd->thd", score_low, key_wide)
    return query_part, key_part, value_part


def reference(queries, out_grad, outputs, key_vectors, value_vectors, logsumexp, positions, doc_start):
    row_delta = jnp.sum(out_grad.astype(jnp.float32) * outputs.astype(jnp.float32), axis=-1)
    query_blocks = queries.reshape(N_BLK, TOK_DEV, HQ, HD)
    grad_blocks = out_grad.reshape(N_BLK, TOK_DEV, HQ, HD)
    norm_blocks = logsumexp.reshape(N_BLK, TOK_DEV, HQ)
    delta_blocks = row_delta.reshape(N_BLK, TOK_DEV, HQ)
    place_blocks = positions.reshape(N_BLK, TOK_DEV)
    start_blocks = doc_start.reshape(N_BLK, TOK_DEV)
    key_blocks = key_vectors.reshape(N_BLK, TOK_DEV, HD)
    value_blocks = value_vectors.reshape(N_BLK, TOK_DEV, HD)
    query_total = jnp.zeros((N_BLK, TOK_DEV, HQ, HD), jnp.float32)
    key_total = jnp.zeros((N_BLK, TOK_DEV, HD), jnp.float32)
    value_total = jnp.zeros((N_BLK, TOK_DEV, HD), jnp.float32)

    def block_pass(inputs):
        return block_grads(*inputs)

    for cycle_step in range(STEPS):
        moved_keys = jnp.roll(key_blocks, -cycle_step, axis=0)
        moved_values = jnp.roll(value_blocks, -cycle_step, axis=0)
        moved_places = jnp.roll(place_blocks, -cycle_step, axis=0)
        query_part, key_part, value_part = lax.map(block_pass, (query_blocks, grad_blocks, norm_blocks, delta_blocks, place_blocks, start_blocks, moved_keys, moved_values, moved_places))
        query_total = query_total + query_part
        key_total = key_total + jnp.roll(key_part, cycle_step, axis=0)
        value_total = value_total + jnp.roll(value_part, cycle_step, axis=0)
    return (query_total.reshape(SEQ, HQ, HD).astype(jnp.bfloat16), key_total.reshape(SEQ, HD).astype(jnp.bfloat16), value_total.reshape(SEQ, HD).astype(jnp.bfloat16))
```

```python
import functools
import math

import jax
import jax.numpy as jnp
from jax import lax
from jax.experimental import pallas as pl
from jax.experimental.pallas import tpu as pltpu
from jax.sharding import PartitionSpec as P

STEPS = 4
TILE = 64
CHUNK = 128
LOG2E = math.log2(math.e)
MESH = pl.DeviceIdType.MESH
VMEM_SPEC = pl.BlockSpec(memory_space=pltpu.VMEM)
ANY_SPEC = pl.BlockSpec(memory_space=pl.ANY)
ROWS = (((1,), (1,)), ((), ()))
COLS = (((0,), (0,)), ((), ()))


def places(n):
    b = lax.axis_index("blk")
    h = lax.axis_index("head")
    even = lax.rem(b, 2) == 0
    partner = jnp.where(even, b + 1, b - 1)

    def at(d):
        return lax.rem(b + d + n, n)

    return b, h, even, partner, at


def greet(n):
    b, h, even, partner, at = places(n)
    barrier = pltpu.get_barrier_semaphore()
    for d in (-3, -2, -1, 1, 2, 3):
        pl.semaphore_signal(barrier, inc=1, device_id=(at(d), h), device_id_type=MESH)
    pl.semaphore_signal(barrier, inc=1, device_id=(b, 1 - h), device_id_type=MESH)
    pl.semaphore_wait(barrier, 7)


def fill_table(table, g_ref, o_ref, lse_ref, start_ref, pos_ref):
    heads, tokens = lse_ref.shape
    block = TILE * heads
    spread = (
        lax.broadcasted_iota(jnp.int32, (TILE, block), 1) // heads
        == lax.broadcasted_iota(jnp.int32, (TILE, block), 0)
    ).astype(jnp.bfloat16)
    choose = (
        lax.broadcasted_iota(jnp.int32, (heads, block), 1) % heads
        == lax.broadcasted_iota(jnp.int32, (heads, block), 0)
    )

    def spread_whole(values):
        upper = values // 256
        lower = values - upper * 256
        up, low = (
            jnp.dot(
                jnp.broadcast_to(part.astype(jnp.float32), (8, TILE)).astype(jnp.bfloat16),
                spread,
                preferred_element_type=jnp.float32,
            )
            for part in (upper, lower)
        )
        return (up * 256.0 + low)[0:1]

    ones = jnp.ones((8, g_ref.shape[1]), jnp.bfloat16)
    for c in range(g_ref.shape[0] // block):
        r = pl.ds(c * block, block)
        product = g_ref[r].astype(jnp.float32) * o_ref[r].astype(jnp.float32)
        upper = product.astype(jnp.bfloat16)
        lower = (product - upper.astype(jnp.float32)).astype(jnp.bfloat16)
        delta = lax.dot_general(
            ones, upper, ROWS, preferred_element_type=jnp.float32
        ) + lax.dot_general(ones, lower, ROWS, preferred_element_type=jnp.float32)
        table[0:1, r] = delta[0:1]
        rest = lse_ref[:, c * TILE : (c + 1) * TILE] * LOG2E
        lse = jnp.zeros((heads, block), jnp.float32)
        for _ in range(3):
            part = rest.astype(jnp.bfloat16)
            rest = rest - part.astype(jnp.float32)
            lse += jnp.dot(part, spread, preferred_element_type=jnp.float32)
        table[1:2, r] = jnp.sum(jnp.where(choose, lse, 0.0), axis=0, keepdims=True)
        at = slice(c * TILE, (c + 1) * TILE)
        table[2:3, r] = spread_whole(start_ref[:, at])
        table[3:4, r] = spread_whole(pos_ref[:, at])


def kernel(
    n, k_hbm, v_hbm, lse_hbm, start_hbm, pos_hbm, q_hbm, g_hbm, o_hbm,
    dq_ref, total, last,
    kv, q_ref, g_ref, o_ref, lse_ref, start_ref, pos_ref, marks, table,
    kp_buf, own_kp, p_buf, ds_buf, dk_acc, dv_acc, dq_acc,
    part, near, mid, guest, extra, send, recv, local,
):
    b, h, even, partner, at = places(n)
    _, tokens, double = kv.shape
    width = double // 2
    heads = lse_ref.shape[0]
    block = TILE * heads
    count = tokens // TILE
    chunks = tokens // CHUNK
    per = CHUNK // TILE
    scaling = width ** (-0.5)
    left, right = slice(0, width), slice(width, double)

    def copy(src, dst, kind, c, who):
        return pltpu.make_async_remote_copy(
            src_ref=src,
            dst_ref=dst,
            send_sem=send.at[kind, c],
            recv_sem=recv.at[kind, c],
            device_id=who,
            device_id_type=MESH,
        )

    loads = [
        pltpu.make_async_copy(src, dst, local.at[j])
        for j, (src, dst) in enumerate(
            (
                (k_hbm, kv.at[0, :, left]),
                (v_hbm, kv.at[0, :, right]),
                (pos_hbm, pos_ref),
                (g_hbm, g_ref),
                (o_hbm, o_ref),
                (lse_hbm, lse_ref),
                (start_hbm, start_ref),
                (q_hbm, q_ref),
            )
        )
    ]
    for c in loads:
        c.start()
    greet(n)

    first, other, fwd, give, own, hop, side = {}, {}, {}, {}, {}, {}, {}
    slot = jnp.where(even, 1, 3)
    flip = jnp.where(even, 3, 1)
    for c in range(chunks):
        r = pl.ds(c * CHUNK, CHUNK)
        first[c] = copy(kv.at[0, r], kv.at[2, r], 0, c, (at(-2), h))
        other[c] = copy(
            kv.at[0, r], kv.at[flip, r], 1, c, (jnp.where(even, at(-3), partner), h)
        )
        fwd[c] = copy(kv.at[2, r], kv.at[slot, r], 2, c, (partner, h))
        give[c] = copy(part.at[flip, r], near.at[r], 3, c, (partner, h))
        own[c] = copy(
            part.at[slot, r], extra.at[r], 4, c, (jnp.where(even, partner, at(3)), h)
        )
        hop[c] = copy(mid.at[r], guest.at[r], 5, c, (at(2), h))
        side[c] = copy(total.at[r], last.at[r], 6, c, (b, 1 - h))
    note = [
        copy(pos_ref.at[:, left], marks.at[d], 7, d, (at(-d), h)) for d in range(1, STEPS)
    ]

    for c in loads[:3]:
        c.wait()
    for c in note:
        c.start()
    for c in reversed(range(chunks)):
        first[c].start()
        other[c].start()

    dq_acc[...] = jnp.zeros_like(dq_acc)
    ramp = lax.broadcasted_iota(jnp.int32, (CHUNK, width), 0) * n
    own_kp[...] = (ramp + pos_ref[0:1, 0:1]).astype(jnp.float32)
    for c in loads[3:7]:
        c.wait()
    fill_table(table, g_ref, o_ref, lse_ref, start_ref, pos_ref)
    loads[7].wait()
    for c in note:
        c.wait()
    for s in range(1, STEPS):
        kp_buf[(s - 1) * TILE : s * TILE, :] = (
            ramp[:TILE] + marks[s, 0:1, 0:1]
        ).astype(jnp.float32)

    def lanes(i):
        if isinstance(i, int):
            return pl.ds(i * block, block)
        return pl.ds(pl.multiple_of(i * block, block), block)

    def keys_of(unit):
        kind, t = unit
        if kind == 0:
            rows = kv[1:STEPS, t * TILE : (t + 1) * TILE, :]
            return rows.reshape((STEPS - 1) * TILE, double), kp_buf, t * (TILE * n)
        return kv[0, t * CHUNK : (t + 1) * CHUNK, :], own_kp, t * (CHUNK * n)

    def probs(unit, i, causal):
        rows, places_of, moved = keys_of(unit)
        r = lanes(i)
        start = table[2:3, r] - float(moved)
        kp = jnp.concatenate([places_of[...]] * (block // width), axis=1)
        s = lax.dot_general(rows[:, left], q_ref[r, :], ROWS, preferred_element_type=jnp.float32)
        dp = lax.dot_general(rows[:, right], g_ref[r, :], ROWS, preferred_element_type=jnp.float32)
        ok = kp >= start
        if causal:
            ok = ok & (kp <= table[3:4, r] - float(moved))
        p = jnp.where(ok, jnp.exp2(s * (scaling * LOG2E) - table[1:2, r]), 0.0)
        return p.astype(jnp.bfloat16), (p * (dp - table[0:1, r])).astype(jnp.bfloat16)

    def put(pair):
        size = pair[0].shape[0]
        p_buf[:size], ds_buf[:size] = pair

    def add_grads(unit, i):
        rows, _, _ = keys_of(unit)
        size = rows.shape[0]
        r = lanes(i)
        ds = ds_buf[:size]
        dv_acc[:size] += jnp.dot(p_buf[:size], g_ref[r, :], preferred_element_type=jnp.float32)
        dk_acc[:size] += jnp.dot(ds, q_ref[r, :], preferred_element_type=jnp.float32)
        dq_acc[:, r] += lax.dot_general(
            rows[:, left], ds, COLS, preferred_element_type=jnp.float32
        )

    def clear():
        dk_acc[...] = jnp.zeros_like(dk_acc)
        dv_acc[...] = jnp.zeros_like(dv_acc)

    def arrive(c):
        other[c].wait_recv()
        fwd[c].wait_recv()

    def relay(c):
        first[c].wait_recv()
        fwd[c].start()

    def merge(c):
        r = pl.ds(c * CHUNK, CHUNK)
        give[c].wait_recv()
        mid[r] = (part[2, r].astype(jnp.float32) + near[r].astype(jnp.float32)).astype(mid.dtype)
        hop[c].start()

    units = [((0, t), t) for t in reversed(range(count))]
    units += [((1, c), c * per) for c in reversed(range(chunks))]

    def after(unit):
        kind, t = unit
        if kind == 0:
            at_rows = slice(t * TILE, (t + 1) * TILE)
            for s in range(1, STEPS):
                mine = slice((s - 1) * TILE, s * TILE)
                part[s, at_rows, left] = (dk_acc[mine] * scaling).astype(part.dtype)
                part[s, at_rows, right] = dv_acc[mine].astype(part.dtype)
            clear()
            c = t // per
            if t % per == 0:
                give[c].start()
                own[c].start()
            elif c + 1 < chunks:
                merge(c + 1)
        else:
            if t == chunks - 1:
                merge(0)
            r = pl.ds(t * CHUNK, CHUNK)
            hop[t].wait_recv()
            own[t].wait_recv()
            both = guest[r].astype(jnp.float32) + extra[r].astype(jnp.float32)
            total[r, left] = (dk_acc[:CHUNK] * scaling + both[:, left]).astype(total.dtype)
            total[r, right] = (dv_acc[:CHUNK] + both[:, right]).astype(total.dtype)
            clear()
            side[t].start()

    clear()
    relay(chunks - 1)
    arrive(chunks - 1)
    put(probs(*units[0], True))
    for j, (unit, low) in enumerate(units):
        kind, t = unit

        def body(i, carry, unit=unit, kind=kind):
            pair = probs(unit, i, kind == 1)
            add_grads(unit, i - 1)
            put(pair)
            return carry

        if low + 1 < count:
            lax.fori_loop(low + 1, count, body, 0)
        if kind == 0 and t > 0:
            if t % per == 0:
                arrive(t // per - 1)
            elif t // per > 0:
                relay(t // per - 1)
        if j + 1 < len(units):
            pair = probs(*units[j + 1], True)
            add_grads(unit, count - 1)
            put(pair)
        else:
            add_grads(unit, count - 1)
        after(unit)

    for i in range(count):
        r = lanes(i)
        dq_ref[r, :] = (dq_acc[:, r].T * scaling).astype(dq_ref.dtype)
    for c in range(chunks):
        for x in (first[c], other[c], fwd[c], give[c], own[c], hop[c]):
            x.wait_send()
        side[c].wait()


def fused(n, k, v, lse, start, pos, q, g, o):
    rows, width = k.shape
    heads = lse.shape[0]
    block = TILE * heads
    keys = max((STEPS - 1) * TILE, CHUNK)
    chunks = rows // CHUNK
    pair = (rows, 2 * width)
    low = jnp.bfloat16
    f32 = jnp.float32
    return pl.pallas_call(
        functools.partial(kernel, n),
        out_shape=(
            jax.ShapeDtypeStruct(q.shape, q.dtype),
            jax.ShapeDtypeStruct(pair, low),
            jax.ShapeDtypeStruct(pair, low),
        ),
        in_specs=[ANY_SPEC] * 8,
        out_specs=(VMEM_SPEC,) * 3,
        scratch_shapes=[
            pltpu.VMEM((STEPS,) + pair, low),
            pltpu.VMEM(q.shape, low),
            pltpu.VMEM(q.shape, low),
            pltpu.VMEM(q.shape, low),
            pltpu.VMEM(lse.shape, f32),
            pltpu.VMEM(start.shape, start.dtype),
            pltpu.VMEM(pos.shape, pos.dtype),
            pltpu.VMEM((STEPS, 1, width), pos.dtype),
            pltpu.VMEM((4, q.shape[0]), f32),
            pltpu.VMEM(((STEPS - 1) * TILE, width), f32),
            pltpu.VMEM((CHUNK, width), f32),
            pltpu.VMEM((keys, block), low),
            pltpu.VMEM((keys, block), low),
            pltpu.VMEM((keys, width), f32),
            pltpu.VMEM((keys, width), f32),
            pltpu.VMEM((width, q.shape[0]), f32),
            pltpu.VMEM((STEPS,) + pair, low),
            pltpu.VMEM(pair, low),
            pltpu.VMEM(pair, low),
            pltpu.VMEM(pair, low),
            pltpu.VMEM(pair, low),
            pltpu.SemaphoreType.DMA((8, max(chunks, STEPS))),
            pltpu.SemaphoreType.DMA((8, max(chunks, STEPS))),
            pltpu.SemaphoreType.DMA((8,)),
        ],
        compiler_params=pltpu.CompilerParams(
            collective_id=0, has_side_effects=True, vmem_limit_bytes=60 << 20
        ),
        name="fused_grads",
    )(k, v, lse, start, pos, q, g, o)


def on_device(
    n, queries, out_grad, outputs, key_vectors, value_vectors, logsumexp, positions, doc_start
):
    width = queries.shape[-1]
    flat = (-1, width)
    dq, total, last = fused(
        n, key_vectors, value_vectors, logsumexp.T, doc_start.reshape(1, -1),
        positions.reshape(1, -1), queries.reshape(flat), out_grad.reshape(flat),
        outputs.reshape(flat),
    )
    both = (total.astype(jnp.float32) + last.astype(jnp.float32)).astype(jnp.bfloat16)
    return dq.reshape(queries.shape), both[:, :width], both[:, width:]


def solution(mesh):
    n = mesh.shape["blk"]
    in_specs = (
        P("blk", "head", None),
        P("blk", "head", None),
        P("blk", "head", None),
        P("blk", None),
        P("blk", None),
        P("blk", "head"),
        P("blk"),
        P("blk"),
    )
    out_specs = (P("blk", "head", None), P("blk", None), P("blk", None))
    return jax.shard_map(
        functools.partial(on_device, n),
        mesh=mesh,
        in_specs=in_specs,
        out_specs=out_specs,
        check_vma=False,
    )
```

```python
import functools
import math

import jax
import jax.numpy as jnp
from jax import lax
from jax.experimental import pallas as pl
from jax.experimental.pallas import tpu as pltpu
from jax.sharding import PartitionSpec as P

STEPS = 4
TILE = 64
CHUNK = 128
MERGED = 2
LOG2E = math.log2(math.e)
MESH = pl.DeviceIdType.MESH
VMEM_SPEC = pl.BlockSpec(memory_space=pltpu.VMEM)
ANY_SPEC = pl.BlockSpec(memory_space=pl.ANY)
ROWS = (((1,), (1,)), ((), ()))
COLS = (((0,), (0,)), ((), ()))


def places(n):
    b = lax.axis_index("blk")
    h = lax.axis_index("head")
    even = lax.rem(b, 2) == 0
    partner = jnp.where(even, b + 1, b - 1)

    def at(d):
        return lax.rem(b + d + n, n)

    return b, h, even, partner, at


def greet(n):
    b, h, even, partner, at = places(n)
    barrier = pltpu.get_barrier_semaphore()
    for d in (-3, -2, -1, 1, 2, 3):
        for p in (h, 1 - h):
            pl.semaphore_signal(barrier, inc=1, device_id=(at(d), p), device_id_type=MESH)
    pl.semaphore_signal(barrier, inc=1, device_id=(b, 1 - h), device_id_type=MESH)
    pl.semaphore_wait(barrier, 13)


def fill_table(table, g_ref, o_ref, lse_ref, start_ref, pos_ref):
    heads, tokens = lse_ref.shape
    block = TILE * heads
    spread = (
        lax.broadcasted_iota(jnp.int32, (TILE, block), 1) // heads
        == lax.broadcasted_iota(jnp.int32, (TILE, block), 0)
    ).astype(jnp.bfloat16)
    choose = (
        lax.broadcasted_iota(jnp.int32, (heads, block), 1) % heads
        == lax.broadcasted_iota(jnp.int32, (heads, block), 0)
    )

    def spread_whole(values):
        upper = values // 256
        lower = values - upper * 256
        up, low = (
            jnp.dot(
                jnp.broadcast_to(part.astype(jnp.float32), (8, TILE)).astype(jnp.bfloat16),
                spread,
                preferred_element_type=jnp.float32,
            )
            for part in (upper, lower)
        )
        return (up * 256.0 + low)[0:1]

    ones = jnp.ones((8, g_ref.shape[1]), jnp.bfloat16)
    for c in range(g_ref.shape[0] // block):
        r = pl.ds(c * block, block)
        product = g_ref[r].astype(jnp.float32) * o_ref[r].astype(jnp.float32)
        upper = product.astype(jnp.bfloat16)
        lower = (product - upper.astype(jnp.float32)).astype(jnp.bfloat16)
        delta = lax.dot_general(
            ones, upper, ROWS, preferred_element_type=jnp.float32
        ) + lax.dot_general(ones, lower, ROWS, preferred_element_type=jnp.float32)
        table[0:1, r] = delta[0:1]
        rest = lse_ref[:, c * TILE : (c + 1) * TILE] * LOG2E
        lse = jnp.zeros((heads, block), jnp.float32)
        for _ in range(3):
            part = rest.astype(jnp.bfloat16)
            rest = rest - part.astype(jnp.float32)
            lse += jnp.dot(part, spread, preferred_element_type=jnp.float32)
        table[1:2, r] = jnp.sum(jnp.where(choose, lse, 0.0), axis=0, keepdims=True)
        at = slice(c * TILE, (c + 1) * TILE)
        table[2:3, r] = spread_whole(start_ref[:, at])
        table[3:4, r] = spread_whole(pos_ref[:, at])


def kernel(
    n, k_hbm, v_hbm, lse_hbm, start_hbm, pos_hbm, q_hbm, g_hbm, o_hbm,
    dq_ref, out_ref,
    kv, q_ref, g_ref, o_ref, lse_ref, start_ref, pos_ref, marks, table,
    kp_buf, own_kp, p_buf, ds_buf, dk_acc, dv_acc, dq_acc,
    part, mine, near, mid, total, last, sums, box, send, recv, local,
):
    b, h, even, partner, at = places(n)
    _, tokens, double = kv.shape
    width = double // 2
    heads = lse_ref.shape[0]
    block = TILE * heads
    count = tokens // TILE
    chunks = tokens // CHUNK
    per = CHUNK // TILE
    scaling = width ** (-0.5)
    left, right = slice(0, width), slice(width, double)
    groups, segs = segments(count)

    def copy(src, dst, out, into, who):
        return pltpu.make_async_remote_copy(
            src_ref=src,
            dst_ref=dst,
            send_sem=send.at[out],
            recv_sem=recv.at[into],
            device_id=who,
            device_id_type=MESH,
        )

    loads = [
        pltpu.make_async_copy(src, dst, local.at[j])
        for j, (src, dst) in enumerate(
            (
                (k_hbm, kv.at[0, :, left]),
                (v_hbm, kv.at[0, :, right]),
                (pos_hbm, pos_ref),
                (g_hbm, g_ref),
                (o_hbm, o_ref),
                (lse_hbm, lse_ref),
                (start_hbm, start_ref),
                (q_hbm, q_ref),
            )
        )
    ]
    for c in loads:
        c.start()
    greet(n)

    slot = jnp.where(even, 1, 3)
    flip = jnp.where(even, 3, 1)
    group_rows, rows_of = (
        [pl.ds(seg[-1] * TILE, len(seg) * TILE) for seg in split] for split in (groups, segs)
    )
    first, other, fwd, give, own, hop, side, straight = ([] for _ in range(8))
    arrived, summed = [], []
    me = (b, h)
    tail = len(segs) - 1
    kinds = (len(groups), len(groups), MERGED, MERGED, len(segs), len(segs), 1)
    base = [sum(kinds[:j]) for j in range(len(kinds))]
    for c, r in enumerate(group_rows):
        first.append(copy(kv.at[0, r], kv.at[2, r], 0, base[0] + c, (at(-2), h)))
        to = (jnp.where(even, at(-3), partner), h)
        other.append(copy(kv.at[0, r], kv.at[flip, r], 1, base[1] + c, to))
        fwd.append(copy(kv.at[2, r], kv.at[slot, r], 2, base[1] + c, (partner, h)))
        arrived.append(copy(kv.at[0:2, r], kv.at[0:2, r], 0, base[1] + c, me))
    for c, r in enumerate(rows_of):
        side.append(copy(total.at[r], last.at[r], 6, base[4] + c, (b, 1 - h)))
        if c >= MERGED:
            planes = (h, 1 - h) if c == tail else (h,)
            straight.append(
                [
                    copy(part.at[s, r], box.at[p, s, r], 8 + p, base[5] + c, (at(s), who))
                    for p, who in enumerate(planes)
                    for s in range(1, STEPS)
                ]
            )
            whole = box.at[0 : len(planes), 1:STEPS, r]
            summed.append(copy(whole, whole, 0, base[5] + c, me))
            continue
        give.append(copy(part.at[flip, r], near.at[r], 3, base[2] + c, (partner, h)))
        to = (jnp.where(even, partner, at(3)), h)
        own.append(copy(part.at[slot, r], sums.at[0, r], 4, base[3] + c, to))
        hop.append(copy(mid.at[r], sums.at[1, r], 5, base[3] + c, (at(2), h)))
        summed.append(copy(sums.at[:, r], sums.at[:, r], 0, base[3] + c, me))
    note = [
        copy(pos_ref.at[:, left], marks.at[d], 7, base[6], (at(-d), h))
        for d in range(1, STEPS)
    ]
    noted = copy(marks.at[1:STEPS], marks.at[1:STEPS], 7, base[6], me)
    merged = pl.ds(segs[MERGED - 1][-1] * TILE, tokens - segs[MERGED - 1][-1] * TILE)
    rest = pl.ds(0, segs[MERGED - 1][-1] * TILE)
    sent = [copy(kv.at[0], kv.at[2], j, 0, me) for j in range(3)]
    sent += [copy(mid.at[merged], near.at[merged], j, 0, me) for j in range(3, 6)]
    sent += [copy(total, last, 6, 0, me), noted]
    sent.append(copy(part.at[1:STEPS, rest], box.at[0, 1:STEPS, rest], 8, 0, me))
    final = rows_of[tail]
    sent.append(copy(part.at[1:STEPS, final], box.at[1, 1:STEPS, final], 9, 0, me))

    for c in loads[:3]:
        c.wait()
    for c in note:
        c.start()
    for x, y in zip(first, other):
        x.start()
        y.start()

    ramp = lax.broadcasted_iota(jnp.int32, (CHUNK, width), 0) * n
    own_kp[...] = (ramp + pos_ref[0:1, 0:1]).astype(jnp.float32)
    for c in loads[3:7]:
        c.wait()
    fill_table(table, g_ref, o_ref, lse_ref, start_ref, pos_ref)
    loads[7].wait()

    def lanes(i):
        return pl.ds(i * block, block)

    def keys_of(unit):
        kind, t = unit
        if kind == 1:
            rows = kv[1:STEPS, t * TILE : (t + 1) * TILE, :]
            return rows.reshape((STEPS - 1) * TILE, double), kp_buf, t * (TILE * n)
        return kv[0, t * CHUNK : (t + 1) * CHUNK, :], own_kp, t * (CHUNK * n)

    def probs(unit, i):
        kind, t = unit
        causal = i < (t + 1) * (per if kind == 0 else 1)
        rows, places_of, moved = keys_of(unit)
        r = lanes(i)
        start = table[2:3, r] - float(moved)
        kp = jnp.concatenate([places_of[...]] * (block // width), axis=1)
        s = lax.dot_general(rows[:, left], q_ref[r, :], ROWS, preferred_element_type=jnp.float32)
        dp = lax.dot_general(rows[:, right], g_ref[r, :], ROWS, preferred_element_type=jnp.float32)
        ok = kp >= start
        if causal:
            ok = ok & (kp <= table[3:4, r] - float(moved))
        p = jnp.where(ok, jnp.exp2(s * (scaling * LOG2E) - table[1:2, r]), 0.0)
        return p.astype(jnp.bfloat16), (p * (dp - table[0:1, r])).astype(jnp.bfloat16)

    def put(pair, turn):
        size = pair[0].shape[0]
        p_buf[turn, :size], ds_buf[turn, :size] = pair

    seen = set()

    def add(ref, index, value, fresh):
        ref[index] = value if fresh else ref[index] + value

    def add_grads(unit, i, turn, fresh):
        rows, _, _ = keys_of(unit)
        size = rows.shape[0]
        r = lanes(i)
        ds = ds_buf[turn, :size]
        dv = jnp.dot(p_buf[turn, :size], g_ref[r, :], preferred_element_type=jnp.float32)
        dk = jnp.dot(ds, q_ref[r, :], preferred_element_type=jnp.float32)
        dq = lax.dot_general(rows[:, left], ds, COLS, preferred_element_type=jnp.float32)
        add(dv_acc, slice(0, size), dv, fresh)
        add(dk_acc, slice(0, size), dk, fresh)
        add(dq_acc, (slice(None), r), dq, i not in seen)
        seen.add(i)

    def arrive(c):
        arrived[c].wait_recv()

    def relay(c):
        first[c].wait_recv()
        fwd[c].start()

    def merge(c):
        r = rows_of[c]
        give[c].wait_recv()
        mid[r] = (part[2, r].astype(jnp.float32) + near[r].astype(jnp.float32)).astype(mid.dtype)
        hop[c].start()

    def settle(c):
        r = rows_of[c]
        if c >= MERGED:
            summed[c].wait_recv()
            near_sum = sum(box[0, s, r].astype(jnp.float32) for s in range(1, STEPS))
            if c == tail:
                far_sum = sum(box[1, s, r].astype(jnp.float32) for s in range(1, STEPS))
                side[c].wait_recv()
                a = total[r].astype(jnp.float32) + near_sum
                out_ref[r] = (a + (last[r].astype(jnp.float32) + far_sum)).astype(out_ref.dtype)
            else:
                total[r] = (mine[r] + near_sum).astype(total.dtype)
                side[c].start()
            return
        summed[c].wait_recv()
        both = sums[1, r].astype(jnp.float32) + sums[0, r].astype(jnp.float32)
        total[r] = (mine[r] + both).astype(total.dtype)
        side[c].start()

    def finish(unit):
        kind, t = unit
        if kind == 0:
            r = pl.ds(t * CHUNK, CHUNK)
            mine[r, left] = dk_acc[:CHUNK] * scaling
            mine[r, right] = dv_acc[:CHUNK]
        else:
            at_rows = slice(t * TILE, (t + 1) * TILE)
            for s in range(1, STEPS):
                rows = slice((s - 1) * TILE, s * TILE)
                part[s, at_rows, left] = (dk_acc[rows] * scaling).astype(part.dtype)
                part[s, at_rows, right] = dv_acc[rows].astype(part.dtype)

    work, acts, ends = [], {}, {}
    for t in reversed(range(chunks)):
        work += [((0, t), i) for i in range(t * per, count)]
    acts[len(work) - 1 - count // 2] = [("relay", 0)]
    acts[len(work) - 1] = [("note", 0), ("relay", 1), ("arrive", 0)]
    begins = {}
    for t in reversed(range(count)):
        begins[t] = len(work)
        work += [((1, t), i) for i in range(t, count)]
        for c, seg in enumerate(segs):
            if seg[-1] == t:
                ends[len(work) - 1] = c
    for c in range(1, len(groups)):
        todo = acts.setdefault(begins[groups[c][0]] - 1, [])
        if c + 1 < len(groups):
            todo.append(("relay", c + 1))
        todo.append(("arrive", c))
        if c == 1:
            todo.append(("mine", tail))
    def act(name, c):
        if name == "note":
            noted.wait_recv()
            for s in range(1, STEPS):
                kp_buf[(s - 1) * TILE : s * TILE, :] = (
                    ramp[:TILE] + marks[s, 0:1, 0:1]
                ).astype(jnp.float32)
        elif name == "mine":
            r = rows_of[c]
            total[r] = mine[r].astype(total.dtype)
            side[c].start()
        elif name == "relay":
            relay(c)
        elif name == "arrive":
            arrive(c)
        else:
            merge(c)

    put(probs(*work[0]), 0)
    for j, (unit, i) in enumerate(work):
        for name, c in acts.get(j, []):
            act(name, c)
        if j + 1 < len(work):
            put(probs(*work[j + 1]), (j + 1) % 2)
        add_grads(unit, i, j % 2, j == 0 or work[j - 1][0] != unit)
        if j + 1 == len(work) or work[j + 1][0] != unit:
            finish(unit)
        if j in ends:
            c = ends[j]
            if c < MERGED:
                give[c].start()
                own[c].start()
            else:
                for x in straight[c - MERGED]:
                    x.start()
            if 0 < c <= MERGED:
                merge(c - 1)

    def write(i):
        r = lanes(i)
        dq_ref[r, :] = (dq_acc[:, r].T * scaling).astype(dq_ref.dtype)

    for i in range(count):
        write(i)
    for c in range(tail + 1):
        settle(c)
    for c, r in enumerate(rows_of[:tail]):
        side[c].wait_recv()
        out_ref[r] = (total[r].astype(jnp.float32) + last[r].astype(jnp.float32)).astype(out_ref.dtype)
    for x in sent:
        x.wait_send()


def segments(count):
    tiles = list(reversed(range(count)))
    arriving = [tiles[:2]] + [[t] for t in tiles[2:-2]] + [tiles[-2:]]
    leaving = [tiles[: count - 5], tiles[count - 5 : count - 3]]
    leaving += [[t] for t in tiles[count - 3 :]]
    return arriving, leaving


def fused(n, k, v, lse, start, pos, q, g, o):
    rows, width = k.shape
    heads = lse.shape[0]
    block = TILE * heads
    keys = max((STEPS - 1) * TILE, CHUNK)
    pair = (rows, 2 * width)
    low = jnp.bfloat16
    f32 = jnp.float32
    groups, segs = segments(rows // TILE)
    landings = 2 * len(groups) + 2 * MERGED + 2 * len(segs) + 1
    k, v, lse, start, pos, q, g, o = (
        pltpu.with_memory_space_constraint(x, pltpu.HBM)
        for x in (k, v, lse, start, pos, q, g, o)
    )
    return pl.pallas_call(
        functools.partial(kernel, n),
        out_shape=(
            jax.ShapeDtypeStruct(q.shape, q.dtype),
            jax.ShapeDtypeStruct(pair, low),
        ),
        in_specs=[ANY_SPEC] * 8,
        out_specs=(VMEM_SPEC, VMEM_SPEC),
        scratch_shapes=[
            pltpu.VMEM((STEPS,) + pair, low),
            pltpu.VMEM(q.shape, low),
            pltpu.VMEM(q.shape, low),
            pltpu.VMEM(q.shape, low),
            pltpu.VMEM(lse.shape, f32),
            pltpu.VMEM(start.shape, start.dtype),
            pltpu.VMEM(pos.shape, pos.dtype),
            pltpu.VMEM((STEPS, 1, width), pos.dtype),
            pltpu.VMEM((4, q.shape[0]), f32),
            pltpu.VMEM(((STEPS - 1) * TILE, width), f32),
            pltpu.VMEM((CHUNK, width), f32),
            pltpu.VMEM((2, keys, block), low),
            pltpu.VMEM((2, keys, block), low),
            pltpu.VMEM((keys, width), f32),
            pltpu.VMEM((keys, width), f32),
            pltpu.VMEM((width, q.shape[0]), f32),
            pltpu.VMEM((STEPS,) + pair, low),
            pltpu.VMEM(pair, f32),
        ]
        + [pltpu.VMEM(pair, low)] * 4
        + [pltpu.VMEM((2,) + pair, low), pltpu.VMEM((2, STEPS) + pair, low)]
        + [pltpu.SemaphoreType.DMA((count,)) for count in (10, landings, 8)],
        compiler_params=pltpu.CompilerParams(
            collective_id=0, has_side_effects=True, vmem_limit_bytes=32 << 20
        ),
        name="fused_grads",
    )(k, v, lse, start, pos, q, g, o)


def on_device(
    n, queries, out_grad, outputs, key_vectors, value_vectors, logsumexp, positions, doc_start
):
    width = queries.shape[-1]
    flat = (-1, width)
    dq, both = fused(
        n, key_vectors, value_vectors, logsumexp.T, doc_start.reshape(1, -1),
        positions.reshape(1, -1), queries.reshape(flat), out_grad.reshape(flat),
        outputs.reshape(flat),
    )
    return dq.reshape(queries.shape), both[:, :width], both[:, width:]


def solution(mesh):
    n = mesh.shape["blk"]
    in_specs = (
        P("blk", "head", None),
        P("blk", "head", None),
        P("blk", "head", None),
        P("blk", None),
        P("blk", None),
        P("blk", "head"),
        P("blk"),
        P("blk"),
    )
    out_specs = (P("blk", "head", None), P("blk", None), P("blk", None))
    return jax.shard_map(
        functools.partial(on_device, n),
        mesh=mesh,
        in_specs=in_specs,
        out_specs=out_specs,
        check_vma=False,
    )
```

```python
import functools
import math

import jax
import jax.numpy as jnp
from jax import lax
from jax.experimental import pallas as pl
from jax.experimental.pallas import tpu as pltpu
from jax.sharding import PartitionSpec as P

STEPS = 4
TILE = 64
CHUNK = 128
MERGED = 2
LOG2E = math.log2(math.e)
MESH = pl.DeviceIdType.MESH
VMEM_SPEC = pl.BlockSpec(memory_space=pltpu.VMEM)
ANY_SPEC = pl.BlockSpec(memory_space=pl.ANY)
ROWS = (((1,), (1,)), ((), ()))
COLS = (((0,), (0,)), ((), ()))


def places(n):
    b = lax.axis_index("blk")
    h = lax.axis_index("head")
    even = lax.rem(b, 2) == 0
    partner = jnp.where(even, b + 1, b - 1)

    def at(d):
        return lax.rem(b + d + n, n)

    return b, h, even, partner, at


def greet(n):
    b, h, even, partner, at = places(n)
    barrier = pltpu.get_barrier_semaphore()
    for d in (-3, -2, -1, 1, 2, 3):
        for p in (h, 1 - h):
            pl.semaphore_signal(barrier, inc=1, device_id=(at(d), p), device_id_type=MESH)
    pl.semaphore_signal(barrier, inc=1, device_id=(b, 1 - h), device_id_type=MESH)
    pl.semaphore_wait(barrier, 13)


def fill_table(table, g_ref, o_ref, lse_ref, start_ref, pos_ref):
    heads, tokens = lse_ref.shape
    block = TILE * heads
    spread = (
        lax.broadcasted_iota(jnp.int32, (TILE, block), 1) // heads
        == lax.broadcasted_iota(jnp.int32, (TILE, block), 0)
    ).astype(jnp.bfloat16)
    choose = (
        lax.broadcasted_iota(jnp.int32, (heads, block), 1) % heads
        == lax.broadcasted_iota(jnp.int32, (heads, block), 0)
    )

    def spread_whole(values):
        upper = values // 256
        lower = values - upper * 256
        up, low = (
            jnp.dot(
                jnp.broadcast_to(part.astype(jnp.float32), (8, TILE)).astype(jnp.bfloat16),
                spread,
                preferred_element_type=jnp.float32,
            )
            for part in (upper, lower)
        )
        return (up * 256.0 + low)[0:1]

    ones = jnp.ones((8, g_ref.shape[1]), jnp.bfloat16)
    for c in range(g_ref.shape[0] // block):
        r = pl.ds(c * block, block)
        product = g_ref[r].astype(jnp.float32) * o_ref[r].astype(jnp.float32)
        upper = product.astype(jnp.bfloat16)
        lower = (product - upper.astype(jnp.float32)).astype(jnp.bfloat16)
        delta = lax.dot_general(
            ones, upper, ROWS, preferred_element_type=jnp.float32
        ) + lax.dot_general(ones, lower, ROWS, preferred_element_type=jnp.float32)
        table[0:1, r] = delta[0:1]
        rest = lse_ref[:, c * TILE : (c + 1) * TILE] * LOG2E
        lse = jnp.zeros((heads, block), jnp.float32)
        for _ in range(3):
            part = rest.astype(jnp.bfloat16)
            rest = rest - part.astype(jnp.float32)
            lse += jnp.dot(part, spread, preferred_element_type=jnp.float32)
        table[1:2, r] = jnp.sum(jnp.where(choose, lse, 0.0), axis=0, keepdims=True)
        at = slice(c * TILE, (c + 1) * TILE)
        table[2:3, r] = spread_whole(start_ref[:, at])
        table[3:4, r] = spread_whole(pos_ref[:, at])


def kernel(
    n, k_hbm, v_hbm, lse_hbm, start_hbm, pos_hbm, q_hbm, g_hbm, o_hbm,
    dq_ref, dk_ref, dv_ref,
    kv, q_ref, g_ref, o_ref, lse_ref, start_ref, pos_ref, marks, table,
    kp_buf, own_kp, p_buf, ds_buf, dk_acc, dv_acc, dq_acc,
    part, mine, near, mid, total, last, sums, box, send, recv, local,
):
    b, h, even, partner, at = places(n)
    _, tokens, double = kv.shape
    width = double // 2
    heads = lse_ref.shape[0]
    block = TILE * heads
    count = tokens // TILE
    chunks = tokens // CHUNK
    per = CHUNK // TILE
    scaling = width ** (-0.5)
    left, right = slice(0, width), slice(width, double)
    groups, segs = segments(count)

    def copy(src, dst, out, into, who):
        return pltpu.make_async_remote_copy(
            src_ref=src,
            dst_ref=dst,
            send_sem=send.at[out],
            recv_sem=recv.at[into],
            device_id=who,
            device_id_type=MESH,
        )

    loads = [
        pltpu.make_async_copy(src, dst, local.at[j])
        for j, (src, dst) in enumerate(
            (
                (k_hbm, kv.at[0, :, left]),
                (v_hbm, kv.at[0, :, right]),
                (pos_hbm, pos_ref),
                (g_hbm, g_ref),
                (o_hbm, o_ref),
                (lse_hbm, lse_ref),
                (start_hbm, start_ref),
                (q_hbm, q_ref),
            )
        )
    ]
    for c in loads:
        c.start()
    greet(n)

    slot = jnp.where(even, 1, 3)
    flip = jnp.where(even, 3, 1)
    group_rows, rows_of = (
        [pl.ds(seg[-1] * TILE, len(seg) * TILE) for seg in split] for split in (groups, segs)
    )
    first, other, fwd, give, own, hop, side, straight = ([] for _ in range(8))
    arrived, summed = [], []
    me = (b, h)
    tail = len(segs) - 1
    kinds = (len(groups), len(groups), MERGED, MERGED, len(segs), len(segs), 1)
    base = [sum(kinds[:j]) for j in range(len(kinds))]
    for c, r in enumerate(group_rows):
        first.append(copy(kv.at[0, r], kv.at[2, r], 0, base[0] + c, (at(-2), h)))
        to = (jnp.where(even, at(-3), partner), h)
        other.append(copy(kv.at[0, r], kv.at[flip, r], 1, base[1] + c, to))
        fwd.append(copy(kv.at[2, r], kv.at[slot, r], 2, base[1] + c, (partner, h)))
        arrived.append(copy(kv.at[0:2, r], kv.at[0:2, r], 0, base[1] + c, me))
    for c, r in enumerate(rows_of):
        side.append(copy(total.at[r], last.at[r], 6, base[4] + c, (b, 1 - h)))
        if c >= MERGED:
            planes = (h, 1 - h) if c == tail else (h,)
            straight.append(
                [
                    copy(part.at[s, r], box.at[p, s, r], 8 + p, base[5] + c, (at(s), who))
                    for p, who in enumerate(planes)
                    for s in range(1, STEPS)
                ]
            )
            whole = box.at[0 : len(planes), 1:STEPS, r]
            summed.append(copy(whole, whole, 0, base[5] + c, me))
            continue
        give.append(copy(part.at[flip, r], near.at[r], 3, base[2] + c, (partner, h)))
        to = (jnp.where(even, partner, at(3)), h)
        own.append(copy(part.at[slot, r], sums.at[0, r], 4, base[3] + c, to))
        hop.append(copy(mid.at[r], sums.at[1, r], 5, base[3] + c, (at(2), h)))
        summed.append(copy(sums.at[:, r], sums.at[:, r], 0, base[3] + c, me))
    note = [
        copy(pos_ref.at[:, left], marks.at[d], 7, base[6], (at(-d), h))
        for d in range(1, STEPS)
    ]
    noted = copy(marks.at[1:STEPS], marks.at[1:STEPS], 7, base[6], me)
    merged = pl.ds(segs[MERGED - 1][-1] * TILE, tokens - segs[MERGED - 1][-1] * TILE)
    rest = pl.ds(0, segs[MERGED - 1][-1] * TILE)
    sent = [copy(kv.at[0], kv.at[2], j, 0, me) for j in range(3)]
    sent += [copy(mid.at[merged], near.at[merged], j, 0, me) for j in range(3, 6)]
    sent += [copy(total, last, 6, 0, me), noted]
    sent.append(copy(part.at[1:STEPS, rest], box.at[0, 1:STEPS, rest], 8, 0, me))
    final = rows_of[tail]
    sent.append(copy(part.at[1:STEPS, final], box.at[1, 1:STEPS, final], 9, 0, me))

    for c in loads[:3]:
        c.wait()
    for c in note:
        c.start()
    first[0].start()
    for x, y in zip(first[1:], other):
        x.start()
        y.start()
    other[-1].start()

    ramp = lax.broadcasted_iota(jnp.int32, (CHUNK, width), 0) * n
    own_kp[...] = (ramp + pos_ref[0:1, 0:1]).astype(jnp.float32)
    for c in loads[3:7]:
        c.wait()
    fill_table(table, g_ref, o_ref, lse_ref, start_ref, pos_ref)
    loads[7].wait()

    def lanes(i):
        return pl.ds(i * block, block)

    def keys_of(unit):
        kind, t = unit
        if kind == 1:
            rows = kv[1:STEPS, t * TILE : (t + 1) * TILE, :]
            return rows.reshape((STEPS - 1) * TILE, double), kp_buf, t * (TILE * n)
        return kv[0, t * CHUNK : (t + 1) * CHUNK, :], own_kp, t * (CHUNK * n)

    def parts_of(unit, i):
        kind, t = unit
        rows, places_of, _ = keys_of(unit)
        if kind == 0 or i > t:
            return [(rows, places_of[...], 0, block)]
        half = TILE // 2
        few = kv[1:STEPS, t * TILE : t * TILE + half, :].reshape((STEPS - 1) * half, double)
        near_places = places_of[...].reshape(STEPS - 1, TILE, width)[:, :half]
        near_places = near_places.reshape((STEPS - 1) * half, width)
        mid_lane = block // 2
        return [(rows, places_of[...], mid_lane, block), (few, near_places, 0, mid_lane)]

    def probs(unit, i):
        kind, t = unit
        causal = i < (t + 1) * (per if kind == 0 else 1)
        moved = keys_of(unit)[2]
        done = []
        for rows, kp, low_lane, high_lane in parts_of(unit, i):
            r = pl.ds(i * block + low_lane, high_lane - low_lane)
            start = table[2:3, r] - float(moved)
            kp = jnp.concatenate([kp] * ((high_lane - low_lane) // width), axis=1)
            s = lax.dot_general(
                rows[:, left], q_ref[r, :], ROWS, preferred_element_type=jnp.float32
            )
            dp = lax.dot_general(
                rows[:, right], g_ref[r, :], ROWS, preferred_element_type=jnp.float32
            )
            ok = kp >= start
            if causal:
                ok = ok & (kp <= table[3:4, r] - float(moved))
            p = jnp.where(ok, jnp.exp2(s * (scaling * LOG2E) - table[1:2, r]), 0.0)
            ds = p * (dp - table[0:1, r])
            done.append((slice(low_lane, high_lane), p.astype(jnp.bfloat16), ds.astype(jnp.bfloat16)))
        return done

    def put(done, turn):
        for at_lanes, p, ds in done:
            p_buf[turn, : p.shape[0], at_lanes] = p
            ds_buf[turn, : ds.shape[0], at_lanes] = ds

    seen = set()

    def add(ref, index, value, fresh):
        ref[index] = value if fresh else ref[index] + value

    def spread_rows(many, few):
        many = many.reshape(STEPS - 1, TILE, width)
        few = few.reshape(STEPS - 1, TILE // 2, width)
        top = many[:, : TILE // 2] + few
        whole = jnp.concatenate([top, many[:, TILE // 2 :]], axis=1)
        return whole.reshape((STEPS - 1) * TILE, width)

    def add_grads(unit, i, turn, fresh):
        sums = []
        for rows, _, low_lane, high_lane in parts_of(unit, i):
            size = rows.shape[0]
            r = pl.ds(i * block + low_lane, high_lane - low_lane)
            p = p_buf[turn, :size, low_lane:high_lane]
            ds = ds_buf[turn, :size, low_lane:high_lane]
            dv = jnp.dot(p, g_ref[r, :], preferred_element_type=jnp.float32)
            dk = jnp.dot(ds, q_ref[r, :], preferred_element_type=jnp.float32)
            dq = lax.dot_general(rows[:, left], ds, COLS, preferred_element_type=jnp.float32)
            add(dq_acc, (slice(None), r), dq, i not in seen)
            sums.append((dv, dk))
        seen.add(i)
        dv, dk = sums[0]
        if len(sums) > 1:
            dv, dk = (spread_rows(x, y) for x, y in zip(*sums))
        size = dv.shape[0]
        add(dv_acc, slice(0, size), dv, fresh)
        add(dk_acc, slice(0, size), dk, fresh)

    def arrive(c):
        arrived[c].wait_recv()

    def relay(c):
        first[c].wait_recv()
        fwd[c].start()

    def merge(c):
        r = rows_of[c]
        give[c].wait_recv()
        mid[r] = (part[2, r].astype(jnp.float32) + near[r].astype(jnp.float32)).astype(mid.dtype)
        hop[c].start()

    def release(r, both):
        dk_ref[r] = both[:, left].astype(dk_ref.dtype)
        dv_ref[r] = both[:, right].astype(dv_ref.dtype)

    def settle(c):
        r = rows_of[c]
        if c >= MERGED:
            summed[c].wait_recv()
            near_sum = sum(box[0, s, r].astype(jnp.float32) for s in range(1, STEPS))
            if c == tail:
                far_sum = sum(box[1, s, r].astype(jnp.float32) for s in range(1, STEPS))
                side[c].wait_recv()
                a = total[r].astype(jnp.float32) + near_sum
                release(r, a + (last[r].astype(jnp.float32) + far_sum))
            else:
                total[r] = (mine[r] + near_sum).astype(total.dtype)
                side[c].start()
            return
        summed[c].wait_recv()
        both = sums[1, r].astype(jnp.float32) + sums[0, r].astype(jnp.float32)
        total[r] = (mine[r] + both).astype(total.dtype)
        side[c].start()

    def finish(unit):
        kind, t = unit
        if kind == 0:
            r = pl.ds(t * CHUNK, CHUNK)
            mine[r, left] = dk_acc[:CHUNK] * scaling
            mine[r, right] = dv_acc[:CHUNK]
        else:
            at_rows = slice(t * TILE, (t + 1) * TILE)
            for s in range(1, STEPS):
                rows = slice((s - 1) * TILE, s * TILE)
                part[s, at_rows, left] = (dk_acc[rows] * scaling).astype(part.dtype)
                part[s, at_rows, right] = dv_acc[rows].astype(part.dtype)

    work, acts, ends = [], {}, {}
    for t in reversed(range(chunks)):
        work += [((0, t), i) for i in range(t * per, count)]
    acts[len(work) - 1 - count // 2] = [("relay", 0)]
    acts[len(work) - 1] = [("note", 0), ("relay", 1), ("arrive", 0)]
    begins = {}
    for t in reversed(range(count)):
        begins[t] = len(work)
        work += [((1, t), i) for i in range(t, count)]
    for c in range(1, len(groups)):
        todo = acts.setdefault(begins[groups[c][0]] - 1, [])
        if c + 1 < len(groups):
            todo.append(("relay", c + 1))
        todo.append(("arrive", c))
        if c == 1:
            todo.append(("mine", tail))
    early = segs[0][-1] - 1
    acts.setdefault(begins[early - 1] - 1, []).append(("leave", 0))
    drained = set()
    for c in range(1, MERGED + 1):
        stop = begins[segs[c][-1] - 1] - 1
        drained.add(stop)
        acts.setdefault(stop, []).extend([("merge", c - 1), ("leave", c)])
    for c in range(MERGED + 1, len(segs)):
        ends_at = begins[segs[c][-1] - 1] - 1 if segs[c][-1] else len(work) - 1
        ends[ends_at] = c

    def act(name, c):
        if name == "note":
            noted.wait_recv()
            for s in range(1, STEPS):
                kp_buf[(s - 1) * TILE : s * TILE, :] = (
                    ramp[:TILE] + marks[s, 0:1, 0:1]
                ).astype(jnp.float32)
        elif name == "mine":
            r = rows_of[c]
            total[r] = mine[r].astype(total.dtype)
            side[c].start()
        elif name == "relay":
            relay(c)
        elif name == "arrive":
            arrive(c)
        elif name == "leave":
            leave(c)
        else:
            merge(c)

    def leave(c):
        if c < MERGED:
            give[c].start()
            own[c].start()
        else:
            for x in straight[c - MERGED]:
                x.start()

    put(probs(*work[0]), 0)
    for j, (unit, i) in enumerate(work):
        fresh = j == 0 or work[j - 1][0] != unit
        done = j + 1 == len(work) or work[j + 1][0] != unit
        if j in drained:
            add_grads(unit, i, j % 2, fresh)
            finish(unit)
        for name, c in acts.get(j, []):
            act(name, c)
        if j + 1 < len(work):
            put(probs(*work[j + 1]), (j + 1) % 2)
        if j not in drained:
            add_grads(unit, i, j % 2, fresh)
            if done:
                finish(unit)
        if j in ends:
            leave(ends[j])

    def write(i):
        r = lanes(i)
        dq_ref[r, :] = (dq_acc[:, r].T * scaling).astype(dq_ref.dtype)

    for i in range(count):
        write(i)
    for c in range(tail + 1):
        settle(c)
    for c, r in enumerate(rows_of[:tail]):
        side[c].wait_recv()
        release(r, total[r].astype(jnp.float32) + last[r].astype(jnp.float32))
    for x in sent:
        x.wait_send()


def segments(count):
    tiles = list(reversed(range(count)))
    arriving = [tiles[:2]] + [[t] for t in tiles[2:-2]] + [tiles[-2:]]
    leaving = [tiles[: count - 5], tiles[count - 5 : count - 3]]
    leaving += [[t] for t in tiles[count - 3 :]]
    return arriving, leaving


def fused(n, k, v, lse, start, pos, q, g, o):
    rows, width = k.shape
    heads = lse.shape[0]
    block = TILE * heads
    keys = max((STEPS - 1) * TILE, CHUNK)
    pair = (rows, 2 * width)
    low = jnp.bfloat16
    f32 = jnp.float32
    groups, segs = segments(rows // TILE)
    landings = 2 * len(groups) + 2 * MERGED + 2 * len(segs) + 1
    k, v, lse, start, pos, q, g, o = (
        pltpu.with_memory_space_constraint(x, pltpu.HBM)
        for x in (k, v, lse, start, pos, q, g, o)
    )
    return pl.pallas_call(
        functools.partial(kernel, n),
        out_shape=(
            jax.ShapeDtypeStruct(q.shape, q.dtype),
            jax.ShapeDtypeStruct(k.shape, low),
            jax.ShapeDtypeStruct(v.shape, low),
        ),
        in_specs=[ANY_SPEC] * 8,
        out_specs=(VMEM_SPEC,) * 3,
        scratch_shapes=[
            pltpu.VMEM((STEPS,) + pair, low),
            pltpu.VMEM(q.shape, low),
            pltpu.VMEM(q.shape, low),
            pltpu.VMEM(q.shape, low),
            pltpu.VMEM(lse.shape, f32),
            pltpu.VMEM(start.shape, start.dtype),
            pltpu.VMEM(pos.shape, pos.dtype),
            pltpu.VMEM((STEPS, 1, width), pos.dtype),
            pltpu.VMEM((4, q.shape[0]), f32),
            pltpu.VMEM(((STEPS - 1) * TILE, width), f32),
            pltpu.VMEM((CHUNK, width), f32),
            pltpu.VMEM((2, keys, block), low),
            pltpu.VMEM((2, keys, block), low),
            pltpu.VMEM((keys, width), f32),
            pltpu.VMEM((keys, width), f32),
            pltpu.VMEM((width, q.shape[0]), f32),
            pltpu.VMEM((STEPS,) + pair, low),
            pltpu.VMEM(pair, f32),
        ]
        + [pltpu.VMEM(pair, low)] * 4
        + [pltpu.VMEM((2,) + pair, low), pltpu.VMEM((2, STEPS) + pair, low)]
        + [pltpu.SemaphoreType.DMA((count,)) for count in (10, landings, 8)],
        compiler_params=pltpu.CompilerParams(
            collective_id=0, has_side_effects=True, vmem_limit_bytes=32 << 20
        ),
        name="fused_grads",
    )(k, v, lse, start, pos, q, g, o)


def put_kernel(*refs):
    count = len(refs) // 2
    sems = refs[-1]
    moves = [
        pltpu.make_async_copy(refs[j], refs[count + j], sems.at[j]) for j in range(count)
    ]
    for x in moves:
        x.start()
    for x in moves:
        x.wait()


def put_out(*arrays):
    return pl.pallas_call(
        put_kernel,
        out_shape=tuple(jax.ShapeDtypeStruct(x.shape, x.dtype) for x in arrays),
        in_specs=[ANY_SPEC] * len(arrays),
        out_specs=(pl.BlockSpec(memory_space=pltpu.HBM),) * len(arrays),
        scratch_shapes=[pltpu.SemaphoreType.DMA((len(arrays),))],
        compiler_params=pltpu.CompilerParams(vmem_limit_bytes=4 << 20),
        name="put_out",
    )(*arrays)


def on_device(
    n, queries, out_grad, outputs, key_vectors, value_vectors, logsumexp, positions, doc_start
):
    width = queries.shape[-1]
    flat = (-1, width)
    dq, dk, dv = put_out(*fused(
        n, key_vectors, value_vectors, logsumexp.T, doc_start.reshape(1, -1),
        positions.reshape(1, -1), queries.reshape(flat), out_grad.reshape(flat),
        outputs.reshape(flat),
    ))
    return dq.reshape(queries.shape), dk, dv


def solution(mesh):
    n = mesh.shape["blk"]
    in_specs = (
        P("blk", "head", None),
        P("blk", "head", None),
        P("blk", "head", None),
        P("blk", None),
        P("blk", None),
        P("blk", "head"),
        P("blk"),
        P("blk"),
    )
    out_specs = (P("blk", "head", None), P("blk", None), P("blk", None))
    return jax.shard_map(
        functools.partial(on_device, n),
        mesh=mesh,
        in_specs=in_specs,
        out_specs=out_specs,
        check_vma=False,
    )
```

```python
import functools
import math

import jax
import jax.numpy as jnp
from jax import lax
from jax.experimental import pallas as pl
from jax.experimental.pallas import tpu as pltpu
from jax.sharding import PartitionSpec as P

STEPS = 4
TILE = 64
CHUNK = 128
MERGED = 2
SOON = 3
LOG2E = math.log2(math.e)
MESH = pl.DeviceIdType.MESH
VMEM_SPEC = pl.BlockSpec(memory_space=pltpu.VMEM)
ANY_SPEC = pl.BlockSpec(memory_space=pl.ANY)
ROWS = (((1,), (1,)), ((), ()))
COLS = (((0,), (0,)), ((), ()))


def places(n):
    b = lax.axis_index("blk")
    h = lax.axis_index("head")
    even = lax.rem(b, 2) == 0
    partner = jnp.where(even, b + 1, b - 1)

    def at(d):
        return lax.rem(b + d + n, n)

    return b, h, even, partner, at


def greet(n):
    b, h, even, partner, at = places(n)
    barrier = pltpu.get_barrier_semaphore()
    for d in (-3, -2, -1, 1, 2, 3):
        for p in (h, 1 - h):
            pl.semaphore_signal(barrier, inc=1, device_id=(at(d), p), device_id_type=MESH)
    pl.semaphore_signal(barrier, inc=1, device_id=(b, 1 - h), device_id_type=MESH)
    pl.semaphore_wait(barrier, 13)


def fill_table(table, g_ref, o_ref, lse_ref, start_ref, pos_ref):
    heads, tokens = lse_ref.shape
    block = TILE * heads
    spread = (
        lax.broadcasted_iota(jnp.int32, (TILE, block), 1) // heads
        == lax.broadcasted_iota(jnp.int32, (TILE, block), 0)
    ).astype(jnp.bfloat16)
    choose = (
        lax.broadcasted_iota(jnp.int32, (heads, block), 1) % heads
        == lax.broadcasted_iota(jnp.int32, (heads, block), 0)
    )

    def spread_whole(values):
        upper = values // 256
        lower = values - upper * 256
        up, low = (
            jnp.dot(
                jnp.broadcast_to(part.astype(jnp.float32), (8, TILE)).astype(jnp.bfloat16),
                spread,
                preferred_element_type=jnp.float32,
            )
            for part in (upper, lower)
        )
        return (up * 256.0 + low)[0:1]

    ones = jnp.ones((8, g_ref.shape[1]), jnp.bfloat16)
    for c in range(g_ref.shape[0] // block):
        r = pl.ds(c * block, block)
        product = g_ref[r].astype(jnp.float32) * o_ref[r].astype(jnp.float32)
        upper = product.astype(jnp.bfloat16)
        lower = (product - upper.astype(jnp.float32)).astype(jnp.bfloat16)
        delta = lax.dot_general(
            ones, upper, ROWS, preferred_element_type=jnp.float32
        ) + lax.dot_general(ones, lower, ROWS, preferred_element_type=jnp.float32)
        table[0:1, r] = delta[0:1]
        rest = lse_ref[:, c * TILE : (c + 1) * TILE] * LOG2E
        lse = jnp.zeros((heads, block), jnp.float32)
        for _ in range(3):
            part = rest.astype(jnp.bfloat16)
            rest = rest - part.astype(jnp.float32)
            lse += jnp.dot(part, spread, preferred_element_type=jnp.float32)
        table[1:2, r] = jnp.sum(jnp.where(choose, lse, 0.0), axis=0, keepdims=True)
        at = slice(c * TILE, (c + 1) * TILE)
        table[2:3, r] = spread_whole(start_ref[:, at])
        table[3:4, r] = spread_whole(pos_ref[:, at])


def kernel(
    n, k_hbm, v_hbm, lse_hbm, start_hbm, pos_hbm, q_hbm, g_hbm, o_hbm,
    dq_ref, dk_ref, dv_ref,
    kv, q_ref, g_ref, o_ref, lse_ref, start_ref, pos_ref, marks, table,
    kp_buf, own_kp, p_buf, ds_buf, dk_acc, dv_acc, dq_acc,
    part, mine, near, mid, total, last, sums, box, send, recv, local,
):
    b, h, even, partner, at = places(n)
    _, tokens, double = kv.shape
    width = double // 2
    heads = lse_ref.shape[0]
    block = TILE * heads
    count = tokens // TILE
    chunks = tokens // CHUNK
    per = CHUNK // TILE
    scaling = width ** (-0.5)
    left, right = slice(0, width), slice(width, double)
    groups, segs = segments(count)

    def copy(src, dst, out, into, who):
        return pltpu.make_async_remote_copy(
            src_ref=src,
            dst_ref=dst,
            send_sem=send.at[out],
            recv_sem=recv.at[into],
            device_id=who,
            device_id_type=MESH,
        )

    loads = [
        pltpu.make_async_copy(src, dst, local.at[j])
        for j, (src, dst) in enumerate(
            (
                (k_hbm, kv.at[0, :, left]),
                (v_hbm, kv.at[0, :, right]),
                (pos_hbm, pos_ref),
                (g_hbm, g_ref),
                (o_hbm, o_ref),
                (lse_hbm, lse_ref),
                (start_hbm, start_ref),
                (q_hbm, q_ref),
            )
        )
    ]
    for c in loads:
        c.start()
    greet(n)

    slot = jnp.where(even, 1, 3)
    flip = jnp.where(even, 3, 1)
    group_rows, rows_of = (
        [pl.ds(seg[-1] * TILE, len(seg) * TILE) for seg in split] for split in (groups, segs)
    )
    first, other, fwd, give, own, hop, side, straight = ([] for _ in range(8))
    arrived, summed = [], []
    me = (b, h)
    tail = len(segs) - 1
    kinds = (len(groups), len(groups), MERGED, MERGED, len(segs), len(segs), 1)
    base = [sum(kinds[:j]) for j in range(len(kinds))]
    for c, r in enumerate(group_rows):
        first.append(copy(kv.at[0, r], kv.at[2, r], 0, base[0] + c, (at(-2), h)))
        to = (jnp.where(even, at(-3), partner), h)
        other.append(copy(kv.at[0, r], kv.at[flip, r], 1, base[1] + c, to))
        fwd.append(copy(kv.at[2, r], kv.at[slot, r], 2, base[1] + c, (partner, h)))
        arrived.append(copy(kv.at[0:2, r], kv.at[0:2, r], 0, base[1] + c, me))
    for c, r in enumerate(rows_of):
        side.append(copy(total.at[r], last.at[r], 6, base[4] + c, (b, 1 - h)))
        if c >= MERGED:
            planes = (h, 1 - h) if c == tail else (h,)
            straight.append(
                [
                    copy(part.at[s, r], box.at[p, s, r], 8 + p, base[5] + c, (at(s), who))
                    for p, who in enumerate(planes)
                    for s in range(1, STEPS)
                ]
            )
            whole = box.at[0 : len(planes), 1:STEPS, r]
            summed.append(copy(whole, whole, 0, base[5] + c, me))
            continue
        give.append(copy(part.at[flip, r], near.at[r], 3, base[2] + c, (partner, h)))
        to = (jnp.where(even, partner, at(3)), h)
        own.append(copy(part.at[slot, r], sums.at[0, r], 4, base[3] + c, to))
        hop.append(copy(mid.at[r], sums.at[1, r], 5, base[3] + c, (at(2), h)))
        summed.append(copy(sums.at[:, r], sums.at[:, r], 0, base[3] + c, me))
    note = [
        copy(pos_ref.at[:, left], marks.at[d], 7, base[6], (at(-d), h))
        for d in range(1, STEPS)
    ]
    noted = copy(marks.at[1:STEPS], marks.at[1:STEPS], 7, base[6], me)
    merged = pl.ds(segs[MERGED - 1][-1] * TILE, tokens - segs[MERGED - 1][-1] * TILE)
    rest = pl.ds(0, segs[MERGED - 1][-1] * TILE)
    sent = [copy(kv.at[0], kv.at[2], j, 0, me) for j in range(3)]
    sent += [copy(mid.at[merged], near.at[merged], j, 0, me) for j in range(3, 6)]
    sent += [copy(total, last, 6, 0, me), noted]
    sent.append(copy(part.at[1:STEPS, rest], box.at[0, 1:STEPS, rest], 8, 0, me))
    final = rows_of[tail]
    sent.append(copy(part.at[1:STEPS, final], box.at[1, 1:STEPS, final], 9, 0, me))

    for c in loads[:3]:
        c.wait()
    for c in note:
        c.start()
    odd = jnp.logical_not(even)
    first[0].start()
    for x, y in zip(first[1:SOON], other):
        x.start()
        y.start()

    @pl.when(even)
    def _():
        for x, y in zip(first[SOON:], other[SOON - 1 :]):
            x.start()
            y.start()
        other[-1].start()

    @pl.when(odd)
    def _():
        for y in other[SOON - 1 :]:
            y.start()


    ramp = lax.broadcasted_iota(jnp.int32, (CHUNK, width), 0) * n
    own_kp[...] = (ramp + pos_ref[0:1, 0:1]).astype(jnp.float32)
    for c in loads[3:7]:
        c.wait()
    fill_table(table, g_ref, o_ref, lse_ref, start_ref, pos_ref)
    loads[7].wait()

    def lanes(i):
        return pl.ds(i * block, block)

    def keys_of(unit):
        kind, t = unit
        if kind == 1:
            rows = kv[1:STEPS, t * TILE : (t + 1) * TILE, :]
            return rows.reshape((STEPS - 1) * TILE, double), kp_buf, t * (TILE * n)
        return kv[0, t * CHUNK : (t + 1) * CHUNK, :], own_kp, t * (CHUNK * n)

    def parts_of(unit, i):
        kind, t = unit
        rows, places_of, _ = keys_of(unit)
        if kind == 0 or i > t:
            return [(rows, places_of[...], 0, block)]
        half = TILE // 2
        few = kv[1:STEPS, t * TILE : t * TILE + half, :].reshape((STEPS - 1) * half, double)
        near_places = places_of[...].reshape(STEPS - 1, TILE, width)[:, :half]
        near_places = near_places.reshape((STEPS - 1) * half, width)
        mid_lane = block // 2
        return [(rows, places_of[...], mid_lane, block), (few, near_places, 0, mid_lane)]

    def probs(unit, i):
        kind, t = unit
        causal = i < (t + 1) * (per if kind == 0 else 1)
        moved = keys_of(unit)[2]
        done = []
        for rows, kp, low_lane, high_lane in parts_of(unit, i):
            r = pl.ds(i * block + low_lane, high_lane - low_lane)
            start = table[2:3, r] - float(moved)
            kp = jnp.concatenate([kp] * ((high_lane - low_lane) // width), axis=1)
            s = lax.dot_general(
                rows[:, left], q_ref[r, :], ROWS, preferred_element_type=jnp.float32
            )
            dp = lax.dot_general(
                rows[:, right], g_ref[r, :], ROWS, preferred_element_type=jnp.float32
            )
            ok = kp >= start
            if causal:
                ok = ok & (kp <= table[3:4, r] - float(moved))
            p = jnp.where(ok, jnp.exp2(s * (scaling * LOG2E) - table[1:2, r]), 0.0)
            ds = p * (dp - table[0:1, r])
            done.append((slice(low_lane, high_lane), p.astype(jnp.bfloat16), ds.astype(jnp.bfloat16)))
        return done

    def put(done, turn):
        for at_lanes, p, ds in done:
            p_buf[turn, : p.shape[0], at_lanes] = p
            ds_buf[turn, : ds.shape[0], at_lanes] = ds

    seen = set()

    def add(ref, index, value, fresh):
        ref[index] = value if fresh else ref[index] + value

    def spread_rows(many, few):
        many = many.reshape(STEPS - 1, TILE, width)
        few = few.reshape(STEPS - 1, TILE // 2, width)
        top = many[:, : TILE // 2] + few
        whole = jnp.concatenate([top, many[:, TILE // 2 :]], axis=1)
        return whole.reshape((STEPS - 1) * TILE, width)

    def add_grads(unit, i, turn, fresh):
        sums = []
        for rows, _, low_lane, high_lane in parts_of(unit, i):
            size = rows.shape[0]
            r = pl.ds(i * block + low_lane, high_lane - low_lane)
            p = p_buf[turn, :size, low_lane:high_lane]
            ds = ds_buf[turn, :size, low_lane:high_lane]
            dv = jnp.dot(p, g_ref[r, :], preferred_element_type=jnp.float32)
            dk = jnp.dot(ds, q_ref[r, :], preferred_element_type=jnp.float32)
            dq = lax.dot_general(rows[:, left], ds, COLS, preferred_element_type=jnp.float32)
            add(dq_acc, (slice(None), r), dq, i not in seen)
            sums.append((dv, dk))
        seen.add(i)
        dv, dk = sums[0]
        if len(sums) > 1:
            dv, dk = (spread_rows(x, y) for x, y in zip(*sums))
        size = dv.shape[0]
        add(dv_acc, slice(0, size), dv, fresh)
        add(dk_acc, slice(0, size), dk, fresh)

    def arrive(c):
        arrived[c].wait_recv()

    def relay(c):
        first[c].wait_recv()
        fwd[c].start()

    def merge(c):
        r = rows_of[c]
        give[c].wait_recv()
        mid[r] = (part[2, r].astype(jnp.float32) + near[r].astype(jnp.float32)).astype(mid.dtype)
        hop[c].start()

    def release(r, both):
        dk_ref[r] = both[:, left].astype(dk_ref.dtype)
        dv_ref[r] = both[:, right].astype(dv_ref.dtype)

    def settle(c):
        r = rows_of[c]
        if c >= MERGED:
            summed[c].wait_recv()
            near_sum = sum(box[0, s, r].astype(jnp.float32) for s in range(1, STEPS))
            if c == tail:
                far_sum = sum(box[1, s, r].astype(jnp.float32) for s in range(1, STEPS))
                side[c].wait_recv()
                a = total[r].astype(jnp.float32) + near_sum
                release(r, a + (last[r].astype(jnp.float32) + far_sum))
            else:
                total[r] = (mine[r] + near_sum).astype(total.dtype)
                side[c].start()
            return
        summed[c].wait_recv()
        both = sums[1, r].astype(jnp.float32) + sums[0, r].astype(jnp.float32)
        total[r] = (mine[r] + both).astype(total.dtype)
        side[c].start()

    def finish(unit):
        kind, t = unit
        if kind == 0:
            r = pl.ds(t * CHUNK, CHUNK)
            mine[r, left] = dk_acc[:CHUNK] * scaling
            mine[r, right] = dv_acc[:CHUNK]
        else:
            at_rows = slice(t * TILE, (t + 1) * TILE)
            for s in range(1, STEPS):
                rows = slice((s - 1) * TILE, s * TILE)
                part[s, at_rows, left] = (dk_acc[rows] * scaling).astype(part.dtype)
                part[s, at_rows, right] = dv_acc[rows].astype(part.dtype)

    work, acts, ends = [], {}, {}
    for t in reversed(range(chunks)):
        work += [((0, t), i) for i in range(t * per, count)]
    acts[len(work) - 1 - count // 2] = [("later", 0), ("relay", 0)]
    acts[len(work) - 1] = [("note", 0), ("relay", 1), ("arrive", 0)]
    begins = {}
    for t in reversed(range(count)):
        begins[t] = len(work)
        work += [((1, t), i) for i in range(t, count)]
    for c in range(1, len(groups)):
        todo = acts.setdefault(begins[groups[c][0]] - 1, [])
        if c + 1 < len(groups):
            todo.append(("relay", c + 1))
        todo.append(("arrive", c))
        if c == 1:
            todo.append(("mine", tail))
    early = segs[0][-1] - 1
    acts.setdefault(begins[early - 1] - 1, []).append(("leave", 0))
    drained = set()
    for c in range(1, MERGED + 1):
        stop = begins[segs[c][-1] - 1] - 1
        drained.add(stop)
        acts.setdefault(stop, []).extend([("merge", c - 1), ("leave", c)])
    for c in range(MERGED + 1, len(segs)):
        ends_at = begins[segs[c][-1] - 1] - 1 if segs[c][-1] else len(work) - 1
        ends[ends_at] = c

    def act(name, c):
        if name == "note":
            noted.wait_recv()
            for s in range(1, STEPS):
                kp_buf[(s - 1) * TILE : s * TILE, :] = (
                    ramp[:TILE] + marks[s, 0:1, 0:1]
                ).astype(jnp.float32)
        elif name == "later":

            @pl.when(odd)
            def _():
                for x in first[SOON:]:
                    x.start()

        elif name == "mine":
            r = rows_of[c]
            total[r] = mine[r].astype(total.dtype)
            side[c].start()
        elif name == "relay":
            relay(c)
        elif name == "arrive":
            arrive(c)
        elif name == "leave":
            leave(c)
        else:
            merge(c)

    def leave(c):
        if c < MERGED:
            give[c].start()
            own[c].start()
        else:
            for x in straight[c - MERGED]:
                x.start()

    put(probs(*work[0]), 0)
    for j, (unit, i) in enumerate(work):
        fresh = j == 0 or work[j - 1][0] != unit
        done = j + 1 == len(work) or work[j + 1][0] != unit
        if j in drained:
            add_grads(unit, i, j % 2, fresh)
            finish(unit)
        for name, c in acts.get(j, []):
            act(name, c)
        if j + 1 < len(work):
            put(probs(*work[j + 1]), (j + 1) % 2)
        if j not in drained:
            add_grads(unit, i, j % 2, fresh)
            if done:
                finish(unit)
        if j in ends:
            leave(ends[j])

    def write(i):
        r = lanes(i)
        dq_ref[r, :] = (dq_acc[:, r].T * scaling).astype(dq_ref.dtype)

    for c in range(MERGED):
        settle(c)
    for i in range(count):
        write(i)
    for c in range(MERGED, tail + 1):
        settle(c)
    for c, r in enumerate(rows_of[:tail]):
        side[c].wait_recv()
        release(r, total[r].astype(jnp.float32) + last[r].astype(jnp.float32))
    for x in sent:
        x.wait_send()


def segments(count):
    tiles = list(reversed(range(count)))
    arriving = [tiles[:2]] + [[t] for t in tiles[2:-2]] + [tiles[-2:]]
    leaving = [tiles[: count - 5], tiles[count - 5 : count - 3]]
    leaving += [[t] for t in tiles[count - 3 :]]
    return arriving, leaving


def fused(n, k, v, lse, start, pos, q, g, o):
    rows, width = k.shape
    heads = lse.shape[0]
    block = TILE * heads
    keys = max((STEPS - 1) * TILE, CHUNK)
    pair = (rows, 2 * width)
    low = jnp.bfloat16
    f32 = jnp.float32
    groups, segs = segments(rows // TILE)
    landings = 2 * len(groups) + 2 * MERGED + 2 * len(segs) + 1
    k, v, lse, start, pos, q, g, o = (
        pltpu.with_memory_space_constraint(x, pltpu.HBM)
        for x in (k, v, lse, start, pos, q, g, o)
    )
    return pl.pallas_call(
        functools.partial(kernel, n),
        out_shape=(
            jax.ShapeDtypeStruct(q.shape, q.dtype),
            jax.ShapeDtypeStruct(k.shape, low),
            jax.ShapeDtypeStruct(v.shape, low),
        ),
        in_specs=[ANY_SPEC] * 8,
        out_specs=(VMEM_SPEC,) * 3,
        scratch_shapes=[
            pltpu.VMEM((STEPS,) + pair, low),
            pltpu.VMEM(q.shape, low),
            pltpu.VMEM(q.shape, low),
            pltpu.VMEM(q.shape, low),
            pltpu.VMEM(lse.shape, f32),
            pltpu.VMEM(start.shape, start.dtype),
            pltpu.VMEM(pos.shape, pos.dtype),
            pltpu.VMEM((STEPS, 1, width), pos.dtype),
            pltpu.VMEM((4, q.shape[0]), f32),
            pltpu.VMEM(((STEPS - 1) * TILE, width), f32),
            pltpu.VMEM((CHUNK, width), f32),
            pltpu.VMEM((2, keys, block), low),
            pltpu.VMEM((2, keys, block), low),
            pltpu.VMEM((keys, width), f32),
            pltpu.VMEM((keys, width), f32),
            pltpu.VMEM((width, q.shape[0]), f32),
            pltpu.VMEM((STEPS,) + pair, low),
            pltpu.VMEM(pair, f32),
        ]
        + [pltpu.VMEM(pair, low)] * 4
        + [pltpu.VMEM((2,) + pair, low), pltpu.VMEM((2, STEPS) + pair, low)]
        + [pltpu.SemaphoreType.DMA((count,)) for count in (10, landings, 8)],
        compiler_params=pltpu.CompilerParams(
            collective_id=0, has_side_effects=True, vmem_limit_bytes=32 << 20
        ),
        name="fused_grads",
    )(k, v, lse, start, pos, q, g, o)


def put_kernel(*refs):
    count = len(refs) // 2
    sems = refs[-1]
    moves = [
        pltpu.make_async_copy(refs[j], refs[count + j], sems.at[j]) for j in range(count)
    ]
    for x in moves:
        x.start()
    for x in moves:
        x.wait()


def put_out(*arrays):
    return pl.pallas_call(
        put_kernel,
        out_shape=tuple(jax.ShapeDtypeStruct(x.shape, x.dtype) for x in arrays),
        in_specs=[ANY_SPEC] * len(arrays),
        out_specs=(pl.BlockSpec(memory_space=pltpu.HBM),) * len(arrays),
        scratch_shapes=[pltpu.SemaphoreType.DMA((len(arrays),))],
        compiler_params=pltpu.CompilerParams(vmem_limit_bytes=4 << 20),
        name="put_out",
    )(*arrays)


def on_device(
    n, queries, out_grad, outputs, key_vectors, value_vectors, logsumexp, positions, doc_start
):
    width = queries.shape[-1]
    flat = (-1, width)
    dq, dk, dv = put_out(*fused(
        n, key_vectors, value_vectors, logsumexp.T, doc_start.reshape(1, -1),
        positions.reshape(1, -1), queries.reshape(flat), out_grad.reshape(flat),
        outputs.reshape(flat),
    ))
    return dq.reshape(queries.shape), dk, dv


def solution(mesh):
    n = mesh.shape["blk"]
    in_specs = (
        P("blk", "head", None),
        P("blk", "head", None),
        P("blk", "head", None),
        P("blk", None),
        P("blk", None),
        P("blk", "head"),
        P("blk"),
        P("blk"),
    )
    out_specs = (P("blk", "head", None), P("blk", None), P("blk", None))
    return jax.shard_map(
        functools.partial(on_device, n),
        mesh=mesh,
        in_specs=in_specs,
        out_specs=out_specs,
        check_vma=False,
    )
```
